256 devices in a mesh: img: 4 (over y_hi, core), txt: 64 (over x, y_lo, z).
Axes of the slice: x: 4, y: 4 (y_hi: 2, y_lo: 2; y = y_hi * 2 + y_lo), z: 8, core: 2. Of those that a mesh axis runs over, the one named last changes fastest.
Arguments:
- queries: bfloat16 [1, 40960, 8192], P(None, 'txt', 'img'), may hold values from -128 to 128
- visual_keys: bfloat16 [1, 512, 8192], P(None, 'img'), may hold values from -5 to 5
- visual_values: bfloat16 [1, 512, 8192], P(None, 'img'), may hold values from -6 to 6
- out_grad: bfloat16 [1, 40960, 8192], P(None, 'txt', 'img'), may hold values from -6 to 6
- gate_value: float32 [1, 64], P(None, 'img'), may hold values from -1.5 to 1.5
- image_order: int32 [1, 8], replicated, may hold values from 0 to 7, as said below
- image_seen: int32 [40960], P('txt'), may hold values from 1 to 8
Outputs:
- query_grad: bfloat16 [1, 40960, 8192], P(None, 'txt', 'img')
- key_grad: float32 [1, 512, 8192], P(None, 'txt', 'img')
- value_grad: float32 [1, 512, 8192], P(None, 'txt', 'img')
The draws below stay inside these ranges and needn't reach their ends.
Inputs may be any that keep to these rules, and one draw needn't show every extreme that they name: `image_order`: each row names every image of 0 to 7 once.
All inputs are finite; a program needn't handle non-finite values.
Results may differ from the reference program's by a relative error of at most 0.0058.
Values may be sent and summed in bfloat16 or wider, within the bound.
A program may use at most 128 MiB of HBM per device.

```python
import math
import jax
import jax.numpy as jnp
from jax import lax

D = 8192
H = 64
HD = 128
LAT = 64
IMAGES = 8
LAYERS = 1
TOK_DEV = 640
TOKENS = 40960
KEYS = 512


def order_table(key):
    row_list = [jax.random.permutation(jax.random.fold_in(key, 100 + layer_index), IMAGES) for layer_index in range(LAYERS)]
    return jnp.stack(row_list).astype(jnp.int32)


def key_table(key):
    normal_table = jnp.clip(jax.random.normal(jax.random.fold_in(key, 7), (LAYERS, KEYS, D), jnp.float32), -5.0, 5.0)
    return normal_table


def draw_image_order(key, part):
    return order_table(key)


def draw_visual_keys(key, part):
    return key_table(key).astype(jnp.bfloat16)


def draw_queries(key, part):
    normal_table = jnp.clip(jax.random.normal(jax.random.fold_in(key, 9), (LAYERS, TOKENS, D), jnp.float32), -5.0, 5.0)
    return normal_table.astype(jnp.bfloat16)


def set_ends(drawn, stream_key, low, largest):
    spot = [jax.random.randint(jax.random.fold_in(stream_key, axis), (), 0, length) for axis, length in enumerate(drawn.shape)]
    widest = drawn.shape.index(max(drawn.shape))
    neighbour = spot[:widest] + [(spot[widest] + 1) % drawn.shape[widest]] + spot[widest + 1:]
    return drawn.at[tuple(spot)].set(low).at[tuple(neighbour)].set(largest)


def shard_levels(rng, dims, split, least, largest):
    def one(dim, shards_of):
        heights = jax.random.uniform(jax.random.fold_in(jax.random.fold_in(rng, 6), dim), (shards_of,), jnp.float32, least / len(split), largest / len(split))
        return jnp.repeat(jnp.exp(heights), dims[dim] // shards_of).reshape((-1,) + (1,) * (len(dims) - dim - 1))

    level = one(*split[0])
    for cut in split[1:]:
        level = level * one(*cut)
    return level


def scatter_about(stream_key, extent, width, most, shards=(), dtype=jnp.bfloat16):
    gain = shard_levels(stream_key, extent, shards, -0.22, 0.18) if shards else 1.0
    entries = jax.random.normal(stream_key, extent, jnp.float32) * width * gain
    return jnp.minimum(jnp.maximum(entries, -most), most).astype(dtype)


def setup_inputs(seed: int = 0) -> dict:
    streams_of = jax.random.split(jax.random.key(seed), 8)
    queries = draw_queries(jax.random.fold_in(streams_of[7], 71), 0)
    visual_keys = draw_visual_keys(jax.random.fold_in(streams_of[7], 71), 0)
    visual_values = scatter_about(streams_of[2], (LAYERS, KEYS, D), 1.0, 6.0, ((1, 4),))
    out_grad = scatter_about(streams_of[3], (LAYERS, TOKENS, D), 1.0, 6.0, ((1, 64), (2, 4)))
    gate_value = jnp.clip(jax.random.uniform(streams_of[4], (LAYERS, H), jnp.float32, -1.5, 1.5) * shard_levels(streams_of[4], (LAYERS, H), ((1, 4),), -0.4, 0.0), -1.5, 1.5)
    image_order = draw_image_order(jax.random.fold_in(streams_of[7], 71), 0)
    image_seen = set_ends(jax.random.randint(streams_of[6], (TOKENS,), 1, IMAGES + 1), jax.random.fold_in(streams_of[6], 1), 1, IMAGES).astype(jnp.int32)
    return dict(queries=queries, visual_keys=visual_keys, visual_values=visual_values, out_grad=out_grad, gate_value=gate_value, image_order=image_order, image_seen=image_seen)


def rounded(array):
    return lax.optimization_barrier(array.astype(jnp.bfloat16)).astype(jnp.float32)

def reference(queries, visual_keys, visual_values, out_grad, gate_value, image_order, image_seen):
    score_scale = 1.0 / math.sqrt(HD)
    block_count = TOKENS // TOK_DEV
    query_list = []
    key_list = []
    value_list = []
    for layer_index in range(LAYERS):
        key_image = jnp.broadcast_to(image_order[layer_index][:, None], (IMAGES, LAT)).reshape(KEYS)
        key_heads = visual_keys[layer_index].astype(jnp.float32).reshape(KEYS, H, HD)
        value_heads = visual_values[layer_index].astype(jnp.float32).reshape(KEYS, H, HD)
        factor = jnp.tanh(gate_value[layer_index])

        def block_step(totals, pieces):
            query_block, grad_block, seen_block = pieces
            query_heads = query_block.astype(jnp.float32).reshape(TOK_DEV, H, HD)
            gated_grad = rounded(grad_block.astype(jnp.float32).reshape(TOK_DEV, H, HD) * factor[None, :, None])
            allowed = key_image[None, :] < seen_block[:, None]
            scores = jnp.einsum('thd,khd->htk', query_heads, key_heads) * score_scale
            masked = jnp.where(allowed[None], scores, -1e+30)
            row_max = lax.optimization_barrier(jnp.max(masked, axis=2, keepdims=True))
            exponent = jnp.where(allowed[None], jnp.exp(masked - row_max), 0.0)
            weights = exponent / lax.optimization_barrier(jnp.sum(exponent, axis=2, keepdims=True))
            weight_half = rounded(weights)
            attended = jnp.einsum('htk,khd->thd', weight_half, value_heads)
            row_delta = lax.optimization_barrier(jnp.sum(gated_grad * attended, axis=2))
            weight_grad = jnp.einsum('thd,khd->htk', gated_grad, value_heads)
            score_half = rounded(weights * (weight_grad - jnp.transpose(row_delta)[:, :, None]))
            query_part = (jnp.einsum('htk,khd->thd', score_half, key_heads) * score_scale).astype(jnp.bfloat16)
            key_part = jnp.einsum('htk,thd->khd', score_half, query_heads) * score_scale
            value_part = jnp.einsum('htk,thd->khd', weight_half, gated_grad)
            new_totals = (totals[0] + key_part.reshape(KEYS, D), totals[1] + value_part.reshape(KEYS, D))
            return (new_totals, query_part.reshape(TOK_DEV, D))
        inputs = (queries[layer_index].reshape(block_count, TOK_DEV, D), out_grad[layer_index].reshape(block_count, TOK_DEV, D), image_seen.reshape(block_count, TOK_DEV))
        empty_sum = jnp.zeros((KEYS, D), jnp.float32)
        sums, query_parts = lax.scan(block_step, (empty_sum, empty_sum), inputs)
        query_list.append(query_parts.reshape(TOKENS, D))
        key_list.append(sums[0])
        value_list.append(sums[1])
    return (jnp.stack(query_list), jnp.stack(key_list), jnp.stack(value_list))
```

```python
import functools
import math

import jax
import jax.numpy as jnp
from jax import lax
from jax.experimental import pallas as pl
from jax.experimental.pallas import tpu as pltpu
from jax.sharding import PartitionSpec as P

MESH = pl.DeviceIdType.MESH
F32, BF16 = jnp.float32, jnp.bfloat16
HEAD = 128
LATENTS = 64
NX, NLO, NZ = 4, 2, 8
GROUP = NLO * NZ


def product(a, b, ca, cb):
    return lax.dot_general(a, b, (((ca,), (cb,)), ((), ())), preferred_element_type=F32)


def kernel(
    chunks, per, q_hbm, k_hbm, v_hbm, g_hbm, gate, order, seen, dq_hbm, kg_ref, vg_ref,
    q_s, g_s, kv_s, dq_s, may_s, part_s, a_s, b_s, bc_s, zs_s, rz_s,
    own_sem, cross_tx, cross_rx, mate_tx, mate_rx, relay_tx, relay_rx,
    first_tx, a_rx, b_tx, bc_rx, z_tx, z_rx, dq_sem,
):
    img, txt = lax.axis_index("img"), lax.axis_index("txt")
    hi, core = img // 2, lax.rem(img, 2)
    x, lo, z = txt // GROUP, lax.rem(txt // NZ, NLO), lax.rem(txt, NZ)
    slot = lax.rem(txt, GROUP)
    tokens, width = q_s.shape
    block = k_hbm.shape[1]
    half = block // 2
    keys = 4 * block
    images = keys // LATENTS
    cw = per * HEAD
    slab = keys // NX
    scale = 1.0 / math.sqrt(HEAD)
    scale2 = scale * math.log2(math.e)

    mate = (hi * 2 + 1 - core, txt)
    flipped = txt + (1 - 2 * lo) * NZ
    cross = [((1 - hi) * 2 + c, flipped) for c in range(2)]
    relay = (img, flipped)
    xp, xm, xo = lax.rem(x + 1, NX), lax.rem(x + NX - 1, NX), lax.rem(x + 2, NX)
    up, down = (img, xp * GROUP + slot), (img, xm * GROUP + slot)

    def in_group(j):
        other = lax.rem(slot + j, GROUP)
        return other, (img, x * GROUP + other)

    def local(src, dst, sem):
        return pltpu.make_async_copy(src, dst, sem)

    def remote(src, dst, tx, rx, to):
        return pltpu.make_async_remote_copy(
            src_ref=src, dst_ref=dst, send_sem=tx, recv_sem=rx, device_id=to, device_id_type=MESH
        )

    def columns(c, base=0):
        return pl.ds(pl.multiple_of(base + c * cw, HEAD), cw)

    def rows(start, size):
        return pl.ds(pl.multiple_of(start, 16), size)

    own_columns = pl.ds(pl.multiple_of(img * width, HEAD), width)
    loads = [
        local(k_hbm.at[0, :, own_columns], kv_s.at[0, img], own_sem.at[0]),
        local(v_hbm.at[0, :, own_columns], kv_s.at[1, img], own_sem.at[1]),
        local(q_hbm.at[0], q_s, own_sem.at[2]),
        local(g_hbm.at[0], g_s, own_sem.at[3]),
    ]
    for copy in loads:
        copy.start()

    barrier = pltpu.get_barrier_semaphore()
    for to in [mate, *cross, up, down]:
        pl.semaphore_signal(barrier, inc=1, device_id=to, device_id_type=MESH)

    def greet(j, carry):
        pl.semaphore_signal(barrier, inc=1, device_id=in_group(j)[1], device_id_type=MESH)
        return carry

    lax.fori_loop(1, GROUP, greet, 0)
    pl.semaphore_wait(barrier, 5 + GROUP - 1)

    def cross_piece(c):
        return kv_s.at[:, pl.ds(2 * (1 - hi), 2), rows(lo * half, half), columns(c)]

    def relay_piece(c):
        return kv_s.at[:, pl.ds(2 * (1 - hi), 2), rows((1 - lo) * half, half), columns(c)]

    def mate_piece(c):
        return kv_s.at[:, hi * 2 + 1 - core, :, columns(c)]

    def send_latents(c, carry):
        for to in cross:
            for a, src in enumerate((k_hbm, v_hbm)):
                remote(
                    src.at[0, rows((1 - lo) * half, half), columns(c, to[0] * width)],
                    kv_s.at[a, img, rows((1 - lo) * half, half), columns(c)],
                    cross_tx.at[c], cross_rx.at[c], to,
                ).start()
        for a, src in enumerate((k_hbm, v_hbm)):
            remote(
                src.at[0, :, columns(c, mate[0] * width)],
                kv_s.at[a, img, :, columns(c)],
                mate_tx.at[c], mate_rx.at[c], mate,
            ).start()
        return carry

    lax.fori_loop(0, chunks, send_latents, 0)

    may_s[...] = jnp.concatenate(
        [jnp.where(order[0, b] < seen[...], 1.0, 0.0) for b in range(images)], axis=0
    )

    def pass_on(c):
        piece = cross_piece(c)
        remote(piece, piece, cross_tx.at[c], cross_rx.at[c], relay).wait_recv()
        remote(piece, piece, relay_tx.at[c], relay_rx.at[c], relay).start()

    def latents_ready(c):
        piece = mate_piece(c)
        remote(piece, piece, mate_tx.at[c], mate_rx.at[c], mate).wait_recv()
        piece = relay_piece(c)
        remote(piece, piece, relay_tx.at[c], relay_rx.at[c], relay).wait_recv()

    def head(c, j):
        h = c * per + j
        cols = pl.ds(pl.multiple_of(h * HEAD, HEAD), HEAD)
        k = kv_s[0, :, :, cols].reshape(keys, HEAD)
        v = kv_s[1, :, :, cols].reshape(keys, HEAD)
        q = q_s[:, cols]
        factor = jnp.tanh(jnp.full((8, HEAD), gate[0, h], F32))[0:1]
        gated = (g_s[:, cols].astype(F32) * factor).astype(BF16)
        may = may_s[...] > 0
        scores = product(k, q, 1, 1).reshape(images, LATENTS, tokens)
        top = jnp.where(may, jnp.max(scores, axis=1), -1e30)
        top = jnp.max(top, axis=0, keepdims=True)
        off = jnp.where(may, top, 1e30)
        exponent = jnp.exp2((scores - off[:, None, :]) * scale2).reshape(keys, tokens)
        weights = exponent * (1.0 / jnp.sum(exponent, axis=0, keepdims=True))
        weight_grad = product(v, gated, 1, 1)
        delta = jnp.sum(weights * weight_grad, axis=0, keepdims=True)
        score_half = (weights * (weight_grad - delta)).astype(BF16)
        weight_half = weights.astype(BF16)
        at = pl.ds(j * HEAD, HEAD)
        value_part = product(weight_half, gated, 1, 0)
        part_s[c, 1, :, :, at] = value_part.astype(BF16).reshape(NX, slab, HEAD)
        key_part = product(score_half, q, 1, 0) * scale
        part_s[c, 0, :, :, at] = key_part.astype(BF16).reshape(NX, slab, HEAD)
        dq_s[:, cols] = (product(score_half, k, 0, 0) * scale).astype(BF16)

    def dq_copy(c):
        return local(dq_s.at[:, columns(c)], dq_hbm.at[0, :, columns(c)], dq_sem.at[c])

    def first_sends(c):
        return [
            remote(part_s.at[c, 0, xo], a_s.at[c, 0], first_tx.at[c], a_rx.at[c], down),
            remote(part_s.at[c, 1, xo], a_s.at[c, 1], first_tx.at[c], a_rx.at[c], up),
            remote(part_s.at[c, 0, xp], bc_s.at[c, 1, 0], first_tx.at[c], bc_rx.at[c], up),
            remote(part_s.at[c, 1, xm], bc_s.at[c, 1, 1], first_tx.at[c], bc_rx.at[c], down),
        ]

    def second_sends(c):
        return [
            remote(b_s.at[c, 0], bc_s.at[c, 0, 0], b_tx.at[c], bc_rx.at[c], down),
            remote(b_s.at[c, 1], bc_s.at[c, 0, 1], b_tx.at[c], bc_rx.at[c], up),
        ]

    def second_hop(c):
        piece = a_s.at[c]
        remote(piece, piece, first_tx.at[c], a_rx.at[c], down).wait_recv()
        b_s[c, 0] = (a_s[c, 0].astype(F32) + part_s[c, 0, xm].astype(F32)).astype(BF16)
        b_s[c, 1] = (a_s[c, 1].astype(F32) + part_s[c, 1, xp].astype(F32)).astype(BF16)

    def x_sum(c):
        piece = bc_s.at[c]
        remote(piece, piece, b_tx.at[c], bc_rx.at[c], down).wait_recv()
        both = [
            (
                part_s[c, a, x].astype(F32) + bc_s[c, 0, a].astype(F32) + bc_s[c, 1, a].astype(F32)
            ).reshape(GROUP, slab // GROUP, cw)
            for a in range(2)
        ]
        zs_s[c] = jnp.concatenate(both, axis=1).astype(BF16)
        rz_s[c, slot] = zs_s[c, slot]

    def spread(c):
        def one(j, carry):
            other, to = in_group(j)
            remote(zs_s.at[c, other], rz_s.at[c, slot], z_tx.at[c], z_rx.at[c], to).start()
            return carry

        lax.fori_loop(1, GROUP, one, 0)

    def others(ref):
        return ref.at[pl.ds(0, GROUP - 1)]

    def finish(c):
        piece = others(rz_s.at[c])
        remote(piece, piece, z_tx.at[c], z_rx.at[c], relay).wait_recv()
        total = jnp.sum(rz_s[c].astype(F32), axis=0)
        mine = slab // GROUP
        kg_ref[0, :, columns(c)] = total[:mine]
        vg_ref[0, :, columns(c)] = total[mine:]

    pass_on(0)
    for copy in loads:
        copy.wait()

    def step(s, carry):
        @pl.when(s + 1 < chunks)
        def _():
            pass_on(s + 1)

        @pl.when(s < chunks)
        def _():
            latents_ready(s)

            def one(j, inner):
                head(s, j)
                return inner

            lax.fori_loop(0, per, one, 0)
            dq_copy(s).start()
            for copy in first_sends(s):
                copy.start()

        @pl.when((s >= 1) & (s < chunks + 1))
        def _():
            second_hop(s - 1)
            for copy in second_sends(s - 1):
                copy.start()

        @pl.when((s >= 2) & (s < chunks + 2))
        def _():
            x_sum(s - 2)
            spread(s - 2)

        @pl.when(s >= 3)
        def _():
            finish(s - 3)

        return carry

    lax.fori_loop(0, chunks + 3, step, 0)

    def settle(c, carry):
        dq_copy(c).wait()
        piece = cross_piece(c)
        remote(piece, piece, cross_tx.at[c], cross_rx.at[c], relay).wait_send()
        remote(piece, piece, relay_tx.at[c], relay_rx.at[c], relay).wait_send()
        piece = mate_piece(c)
        remote(piece, piece, mate_tx.at[c], mate_rx.at[c], mate).wait_send()
        piece = bc_s.at[c]
        remote(piece, piece, first_tx.at[c], bc_rx.at[c], down).wait_send()
        piece = b_s.at[c]
        remote(piece, piece, b_tx.at[c], bc_rx.at[c], down).wait_send()
        piece = others(zs_s.at[c])
        remote(piece, piece, z_tx.at[c], z_rx.at[c], relay).wait_send()
        return carry

    lax.fori_loop(0, chunks, settle, 0)


def shards(queries, visual_keys, visual_values, out_grad, gate_value, image_order, image_seen):
    _, tokens, width = queries.shape
    block = visual_keys.shape[1]
    keys = 4 * block
    heads = width // HEAD
    per = 2
    chunks = heads // per
    cw = per * HEAD
    slab = keys // NX
    mine = slab // GROUP
    hbm = pl.BlockSpec(memory_space=pl.ANY)
    vmem = pl.BlockSpec(memory_space=pltpu.VMEM)
    smem = pl.BlockSpec(memory_space=pltpu.SMEM)
    dma = pltpu.SemaphoreType.DMA
    return tuple(
        pl.pallas_call(
            functools.partial(kernel, chunks, per),
            out_shape=(
                jax.ShapeDtypeStruct((1, tokens, width), BF16),
                jax.ShapeDtypeStruct((1, mine, width), F32),
                jax.ShapeDtypeStruct((1, mine, width), F32),
            ),
            in_specs=[hbm, hbm, hbm, hbm, smem, smem, vmem],
            out_specs=(hbm, vmem, vmem),
            scratch_shapes=[
                pltpu.VMEM((tokens, width), BF16),
                pltpu.VMEM((tokens, width), BF16),
                pltpu.VMEM((2, 4, block, width), BF16),
                pltpu.VMEM((tokens, width), BF16),
                pltpu.VMEM((keys // LATENTS, tokens), F32),
                pltpu.VMEM((chunks, 2, NX, slab, cw), BF16),
                pltpu.VMEM((chunks, 2, slab, cw), BF16),
                pltpu.VMEM((chunks, 2, slab, cw), BF16),
                pltpu.VMEM((chunks, 2, 2, slab, cw), BF16),
                pltpu.VMEM((chunks, GROUP, 2 * mine, cw), BF16),
                pltpu.VMEM((chunks, GROUP, 2 * mine, cw), BF16),
                dma((4,)),
            ]
            + [dma((chunks,))] * 13,
            compiler_params=pltpu.CompilerParams(
                collective_id=0, has_side_effects=True, vmem_limit_bytes=60 * 2**20
            ),
            name="attention_grads",
        )(
            queries, visual_keys, visual_values, out_grad, gate_value, image_order,
            image_seen.reshape(1, tokens),
        )
    )


def solution(mesh):
    placed = (
        P(None, "txt", "img"),
        P(None, "img", None),
        P(None, "img", None),
        P(None, "txt", "img"),
        P(None, "img"),
        P(),
        P("txt"),
    )
    return jax.shard_map(
        shards,
        mesh=mesh,
        in_specs=placed,
        out_specs=(P(None, "txt", "img"), P(None, "txt", "img"), P(None, "txt", "img")),
        check_vma=False,
    )
```

```python
import functools
import math
from typing import NamedTuple, Any

import jax
import jax.numpy as jnp
from jax import lax
from jax.experimental import pallas as pl
from jax.experimental.pallas import tpu as pltpu
from jax.sharding import PartitionSpec as P

MESH = pl.DeviceIdType.MESH
F32, BF16 = jnp.float32, jnp.bfloat16
HEAD = 128
LATENTS = 64
NX, NLO, NZ = 4, 2, 8
GROUP = NLO * NZ
PAIR, SECOND, THIRD = 2, 2, 4
PAIRED = (1, 3, 5)
LAST_SECOND, LAST_THIRD = (9, 10), (11, 11)


class Unit(NamedTuple):
    chunk: Any
    cols: Any
    sem: Any
    whole: bool


def product(a, b, ca, cb):
    return lax.dot_general(a, b, (((ca,), (cb,)), ((), ())), preferred_element_type=F32)


def kernel(
    chunks, per, q_hbm, k_hbm, v_hbm, g_hbm, gate, order, seen_hbm, dq_hbm, kg_hbm, vg_hbm,
    q_s, g_s, seen_s, stage_s, kv_s, dq_s, may_s, part_s, pair_s, a_s, b_s, bc_s, zs_s, rz_s, kg_s, vg_s,
    own_sem, round_sem, cross_tx, cross_rx, mate_tx, mate_rx, relay_tx, relay_rx,
    pair_tx, pair_rx, first_tx, a_rx, b_tx, bc_rx, z_tx, z_rx, dq_sem, grad_sem,
):
    img, txt = lax.axis_index("img"), lax.axis_index("txt")
    hi, core = img // 2, lax.rem(img, 2)
    x, lo, z = txt // GROUP, lax.rem(txt // NZ, NLO), lax.rem(txt, NZ)
    slot = lax.rem(txt, GROUP)
    zq, zp = z // 2, lax.rem(z, 2)
    mine = zp * (GROUP // 2) + lo * (NZ // 2) + zq
    tokens, width = q_s.shape
    block = k_hbm.shape[1]
    half = block // 2
    keys = 4 * block
    images = keys // LATENTS
    cw = per * HEAD
    heads = chunks * per
    part = keys // (2 * NX)
    scale = 1.0 / math.sqrt(HEAD)
    scale2 = scale * math.log2(math.e)

    mate = (hi * 2 + 1 - core, txt)
    flipped = txt + (1 - 2 * lo) * NZ
    cross = [((1 - hi) * 2 + c, flipped) for c in range(2)]
    relay = (img, flipped)
    xp, xm, xo = lax.rem(x + 1, NX), lax.rem(x + NX - 1, NX), lax.rem(x + 2, NX)
    up, down = (img, xp * GROUP + slot), (img, xm * GROUP + slot)

    before, after = (img, txt - z + lax.rem(z + NZ - 1, NZ)), (img, txt - z + lax.rem(z + 1, NZ))

    def at_place(g):
        other = lax.rem(g // (NZ // 2), NLO) * NZ + lax.rem(g, NZ // 2) * 2 + g // (GROUP // 2)
        return (img, x * GROUP + other)

    def local(src, dst, sem):
        return pltpu.make_async_copy(src, dst, sem)

    def remote(src, dst, tx, rx, to):
        return pltpu.make_async_remote_copy(
            src_ref=src, dst_ref=dst, send_sem=tx, recv_sem=rx, device_id=to, device_id_type=MESH
        )

    def columns(c, base=0):
        return pl.ds(pl.multiple_of(base + c * cw, HEAD), cw)

    def rows(start, size):
        return pl.ds(pl.multiple_of(start, 16), size)

    barrier = pltpu.get_barrier_semaphore()
    near = [mate, *cross, relay, up, down, before, after]
    for to in near:
        pl.semaphore_signal(barrier, inc=1, device_id=to, device_id_type=MESH)
    own_columns = pl.ds(pl.multiple_of(img * width, HEAD), width)
    staged = [
        local(k_hbm.at[0], stage_s.at[0], own_sem.at[0]),
        local(v_hbm.at[0], stage_s.at[1], own_sem.at[1]),
    ]
    loads = [
        local(k_hbm.at[0, :, own_columns], kv_s.at[0, img], own_sem.at[2]),
        local(v_hbm.at[0, :, own_columns], kv_s.at[1, img], own_sem.at[3]),
        local(seen_hbm, seen_s, own_sem.at[4]),
        local(q_hbm.at[0], q_s, own_sem.at[5]),
        local(g_hbm.at[0], g_s, own_sem.at[6]),
    ]
    for copy in staged + loads:
        copy.start()
    for copy in staged:
        copy.wait()
    pl.semaphore_wait(barrier, len(near))

    def tell(r):
        pl.semaphore_signal(round_sem.at[r, 0], inc=1, device_id=after, device_id_type=MESH)
        pl.semaphore_signal(round_sem.at[r, 1], inc=1, device_id=before, device_id_type=MESH)

    def hear(r):
        pl.semaphore_wait(round_sem.at[r, 0], 1)
        pl.semaphore_wait(round_sem.at[r, 1], 1)

    tell(0)

    def one_head(h, base=0):
        return pl.ds(pl.multiple_of(base + h * HEAD, HEAD), HEAD)

    def cross_piece(h):
        return kv_s.at[:, pl.ds(2 * (1 - hi), 2), rows(lo * half, half), one_head(h)]

    def relay_piece(h):
        return kv_s.at[:, pl.ds(2 * (1 - hi), 2), rows((1 - lo) * half, half), one_head(h)]

    def mate_piece(h):
        return kv_s.at[:, hi * 2 + 1 - core, :, one_head(h)]

    def cross_send(h, to):
        sent = rows((1 - lo) * half, half)
        return remote(
            stage_s.at[:, sent, one_head(h, to[0] * width)], kv_s.at[:, img, sent, one_head(h)],
            cross_tx.at[h], cross_rx.at[h], to,
        )

    def mate_send(h):
        return remote(
            stage_s.at[:, :, one_head(h, mate[0] * width)], kv_s.at[:, img, :, one_head(h)],
            mate_tx.at[h], mate_rx.at[h], mate,
        )

    def send_latents(h, carry):
        for to in cross:
            cross_send(h, to).start()
        mate_send(h).start()
        return carry

    lax.fori_loop(0, heads, send_latents, 0)
    hear(0)
    tell(1)
    for copy in loads:
        copy.wait()
    may_s[...] = jnp.concatenate(
        [jnp.where(order[0, b] < seen_s[...].reshape(1, tokens), 1.0, 0.0) for b in range(images)],
        axis=0,
    )

    def pass_on(h):
        piece = cross_piece(h)
        remote(piece, piece, cross_tx.at[h], cross_rx.at[h], relay).wait_recv()
        remote(piece, piece, relay_tx.at[h], relay_rx.at[h], relay).start()

    def latents_ready(h):
        piece = mate_piece(h)
        remote(piece, piece, mate_tx.at[h], mate_rx.at[h], mate).wait_recv()

        piece = relay_piece(h)
        remote(piece, piece, relay_tx.at[h], relay_rx.at[h], relay).wait_recv()

    def keep(c, a, at, value):
        by_parity = value.reshape(keys // 16, 2, 8, HEAD)
        for p in range(2):
            rows_p = by_parity[:, p].reshape(NX, part, HEAD)
            part_s[c, p, a, :, :, at] = rows_p.astype(BF16)

    def head(c, j):
        h = c * per + j
        cols = pl.ds(pl.multiple_of(h * HEAD, HEAD), HEAD)
        k = kv_s[0, :, :, cols].reshape(keys, HEAD)
        v = kv_s[1, :, :, cols].reshape(keys, HEAD)
        q = q_s[:, cols]
        factor = jnp.tanh(jnp.full((8, HEAD), gate[0, h], F32))[0:1]
        gated = (g_s[:, cols].astype(F32) * factor).astype(BF16)
        may = may_s[...] > 0
        scores = product(k, q, 1, 1).reshape(images, LATENTS, tokens)
        top = jnp.where(may, jnp.max(scores, axis=1), -1e30)
        top = jnp.max(top, axis=0, keepdims=True)
        off = jnp.where(may, top, 1e30)
        exponent = jnp.exp2((scores - off[:, None, :]) * scale2).reshape(keys, tokens)
        weights = exponent * (1.0 / jnp.sum(exponent, axis=0, keepdims=True))
        weight_grad = product(v, gated, 1, 1)
        delta = jnp.sum(weights * weight_grad, axis=0, keepdims=True)
        score_half = (weights * (weight_grad - delta)).astype(BF16)
        weight_half = weights.astype(BF16)
        at = pl.ds(j * HEAD, HEAD)
        keep(c, 1, at, product(weight_half, gated, 1, 0))
        keep(c, 0, at, product(score_half, q, 1, 0) * scale)
        dq_s[:, cols] = (product(score_half, k, 0, 0) * scale).astype(BF16)

    def dq_copy(c):
        return local(dq_s.at[:, columns(c)], dq_hbm.at[0, :, columns(c)], dq_sem.at[c])

    def pair_of(c):
        odd = lax.rem(c // 2, 2)
        return jnp.where(zp == odd, 1, -1)

    def pair_send(u):
        c = u.chunk
        to = (img, txt - z + lax.rem(z + NZ + pair_of(c), NZ))
        return remote(part_s.at[c, 1 - zp], pair_s.at[c], pair_tx.at[c], pair_rx.at[c], to)

    def pair_sum(u):
        c = u.chunk
        pair_send(u).wait_recv()
        for a in range(2):
            for i in range(NX):
                both = part_s[c, zp, a, i].astype(F32) + pair_s[c, a, i].astype(F32)
                part_s[c, zp, a, i] = both.astype(BF16)

    def parities(u):
        return pl.ds(0, 2) if u.whole else pl.ds(0, 1)

    def slab_of(u, a, i):
        return part_s.at[u.chunk, pl.ds(0, 2) if u.whole else pl.ds(zp, 1), a, i, :, u.cols]

    def a_of(u, a):
        return a_s.at[u.chunk, a, parities(u), :, u.cols]

    def b_of(u, a):
        return b_s.at[u.chunk, a, parities(u), :, u.cols]

    def bc_of(u, hop, a):
        return bc_s.at[u.chunk, hop, a, parities(u), :, u.cols]

    both_arrays = pl.ds(0, 2)

    def first_sends(u):
        tx, rx_a, rx_c = first_tx.at[u.sem], a_rx.at[u.sem], bc_rx.at[u.sem]
        return [
            remote(slab_of(u, 0, xo), a_of(u, 0), tx, rx_a, down),
            remote(slab_of(u, 1, xo), a_of(u, 1), tx, rx_a, up),
            remote(slab_of(u, 0, xp), bc_of(u, 1, 0), tx, rx_c, up),
            remote(slab_of(u, 1, xm), bc_of(u, 1, 1), tx, rx_c, down),
        ]

    def second_sends(u):
        return [
            remote(b_of(u, a), bc_of(u, 0, a), b_tx.at[u.sem], bc_rx.at[u.sem], to)
            for a, to in enumerate((down, up))
        ]

    def second_hop(u):
        piece = a_of(u, both_arrays)
        remote(piece, piece, first_tx.at[u.sem], a_rx.at[u.sem], down).wait_recv()
        for a, i in enumerate((xm, xp)):
            for p in range(2 if u.whole else 1):
                own = part_s[u.chunk, p if u.whole else zp, a, i, :, u.cols].astype(F32)
                total = a_s[u.chunk, a, p, :, u.cols].astype(F32) + own
                b_s[u.chunk, a, p, :, u.cols] = total.astype(BF16)

    def x_sum(u):
        piece = bc_of(u, pl.ds(0, 2), both_arrays)
        remote(piece, piece, b_tx.at[u.sem], bc_rx.at[u.sem], down).wait_recv()
        c = u.chunk
        for p in range(2 if u.whole else 1):
            parity = p if u.whole else zp
            both = [
                (
                    part_s[c, parity, a, x, :, u.cols].astype(F32)
                    + bc_s[c, 0, a, p, :, u.cols].astype(F32)
                    + bc_s[c, 1, a, p, :, u.cols].astype(F32)
                ).reshape(GROUP // 2, 8, u.cols.size)
                for a in range(2)
            ]
            places = pl.ds(parity * (GROUP // 2), GROUP // 2)
            zs_s[c, places, :, u.cols] = jnp.concatenate(both, axis=1).astype(BF16)
        rz_s[c, mine, :, u.cols] = zs_s[c, mine, :, u.cols]

    def spread(u):
        size = GROUP if u.whole else GROUP // 2

        def one(j, carry):
            if u.whole:
                g = lax.rem(mine + j, GROUP)
            else:
                g = zp * size + lax.rem(mine + j, size)
            remote(
                zs_s.at[u.chunk, g, :, u.cols], rz_s.at[u.chunk, mine, :, u.cols],
                z_tx.at[u.sem], z_rx.at[u.sem], at_place(g),
            ).start()
            return carry

        lax.fori_loop(1, size, one, 0)

    def others(ref, u):
        return ref.at[u.chunk, pl.ds(0, (GROUP if u.whole else GROUP // 2) - 1), :, u.cols]

    def finish(u):
        piece = others(rz_s, u)
        remote(piece, piece, z_tx.at[u.sem], z_rx.at[u.sem], relay).wait_recv()
        places = pl.ds(0, GROUP) if u.whole else pl.ds(zp * (GROUP // 2), GROUP // 2)
        total = jnp.sum(rz_s[u.chunk, places, :, u.cols].astype(F32), axis=0)
        at = grad_columns(u)
        kg_s[:, at] = total[:8]
        vg_s[:, at] = total[8:]
        for copy in grad_copies(at, u.sem):
            copy.start()

    def grad_columns(u):
        if isinstance(u.chunk, int):
            return pl.ds(u.chunk * cw + u.cols.start, u.cols.size)
        return columns(u.chunk)

    def grad_copies(at, sem):
        return [
            local(kg_s.at[:, at], kg_hbm.at[0, :, at], grad_sem.at[sem, 0]),
            local(vg_s.at[:, at], vg_hbm.at[0, :, at], grad_sem.at[sem, 1]),
        ]

    def start(copies):
        for copy in copies:
            copy.start()

    def after_compute(u):
        if u.whole:
            start(first_sends(u))
        else:
            pair_send(u).start()

    def first_stage(u):
        pair_sum(u)
        start(first_sends(u))

    def second_stage(u):
        second_hop(u)
        start(second_sends(u))

    def third_stage(u):
        x_sum(u)
        spread(u)

    def unit(c, whole):
        return Unit(c, pl.ds(0, cw), c, whole)

    last = chunks - 1
    ends = [Unit(last, pl.ds(j * HEAD, HEAD), last + j, True) for j in range(per)]

    def paired(c):
        return functools.reduce(lambda t, d: t | (c == d), PAIRED, c < 0)

    def each(c, act, forms=(True, False)):
        for whole in forms:
            fits = (c >= 0) & (c < last) & (paired(c) != whole)
            pl.when(fits)(functools.partial(act, unit(c, whole)))

    def compute(h, c, j):
        @pl.when(h + 2 < heads)
        def _():
            pass_on(h + 2)

        latents_ready(h)
        head(c, j)

    hear(1)
    tell(2)
    pass_on(0)
    hear(2)
    tell(3)
    pass_on(1)

    def step(s, carry):
        def one(j, inner):
            compute(s * per + j, s, j)
            return inner

        lax.fori_loop(0, per, one, 0)
        dq_copy(s).start()
        each(s, after_compute)
        pl.when(s == 0)(lambda: hear(3))
        each(s - PAIR, first_stage, (False,))
        each(s - SECOND, second_stage, (True,))
        each(s - PAIR - SECOND, second_stage, (False,))
        each(s - THIRD, third_stage, (True,))
        each(s - PAIR - THIRD, third_stage, (False,))
        return carry

    lax.fori_loop(0, last, step, 0)
    for j, u in enumerate(ends):
        compute(last * per + j, last, j)
        after_compute(u)

    dq_copy(last).start()

    due = {}
    for c in range(last):
        late = PAIR if c in PAIRED else 0
        for at, act in ((0, first_stage), (SECOND, second_stage), (THIRD, third_stage)):
            if c + late + at >= last and (at or late):
                due.setdefault(c + late + at, []).append((act, unit(c, c not in PAIRED)))
    for u, second, third in zip(ends, LAST_SECOND, LAST_THIRD):
        due.setdefault(second, []).append((second_stage, u))
        due.setdefault(third, []).append((third_stage, u))
    def settle_head(h, carry):
        piece = cross_piece(h)
        remote(piece, piece, cross_tx.at[h], cross_rx.at[h], relay).wait_send()
        remote(piece, piece, relay_tx.at[h], relay_rx.at[h], relay).wait_send()
        mate_send(h).wait_send()
        return carry

    def settle_unit(u):
        if not u.whole:
            pair_send(u).wait_send()
        piece = bc_of(u, pl.ds(0, 2), both_arrays)
        remote(piece, piece, first_tx.at[u.sem], bc_rx.at[u.sem], down).wait_send()
        piece = b_of(u, both_arrays)
        remote(piece, piece, b_tx.at[u.sem], bc_rx.at[u.sem], down).wait_send()
        piece = others(zs_s, u)
        remote(piece, piece, z_tx.at[u.sem], z_rx.at[u.sem], relay).wait_send()

    def settle_grads(u):
        for copy in grad_copies(grad_columns(u), u.sem):
            copy.wait()

    def settle(c, carry):
        dq_copy(c).wait()
        each(c, settle_unit)
        return carry

    def settle_all_grads(c, carry):
        each(c, settle_grads)
        return carry

    for s in sorted(due):
        for act, u in due[s]:
            act(u)
        if s == last:
            lax.fori_loop(0, heads, settle_head, 0)

    def end(c, carry):
        each(c, finish)
        return carry

    lax.fori_loop(0, last - 1, settle, 0)
    lax.fori_loop(0, last, end, 0)
    for u in ends:
        finish(u)
    lax.fori_loop(last - 1, chunks, settle, 0)
    lax.fori_loop(0, last, settle_all_grads, 0)
    for u in ends:
        settle_unit(u)
        settle_grads(u)


def hand_on(dq_in, kg_in, vg_in, dq_out, kg_out, vg_out, dq_s, grad_s, sem):
    steps = dq_s.shape[0]
    rows = dq_s.shape[1]
    pairs = [
        (dq_in.at[0, pl.ds(i * rows, rows)], dq_s.at[i], dq_out.at[0, pl.ds(i * rows, rows)])
        for i in range(steps)
    ]
    pairs += [(kg_in.at[0], grad_s.at[0], kg_out.at[0]), (vg_in.at[0], grad_s.at[1], vg_out.at[0])]
    loads = [pltpu.make_async_copy(a, b, sem.at[0, i]) for i, (a, b, _) in enumerate(pairs)]
    stores = [pltpu.make_async_copy(b, c, sem.at[1, i]) for i, (_, b, c) in enumerate(pairs)]
    for copy in loads:
        copy.start()
    for load, store in zip(loads, stores):
        load.wait()
        store.start()
    for copy in stores:
        copy.wait()


def shards(queries, visual_keys, visual_values, out_grad, gate_value, image_order, image_seen):
    _, tokens, width = queries.shape
    block = visual_keys.shape[1]
    keys = 4 * block
    heads = width // HEAD
    per = 2
    chunks = heads // per
    cw = per * HEAD
    part = keys // (2 * NX)
    mine = keys // (NX * GROUP)
    hbm = pl.BlockSpec(memory_space=pl.ANY)
    smem = pl.BlockSpec(memory_space=pltpu.SMEM)
    dma = pltpu.SemaphoreType.DMA
    outs = tuple(
        pl.pallas_call(
            functools.partial(kernel, chunks, per),
            out_shape=(
                jax.ShapeDtypeStruct((1, tokens, width), BF16),
                jax.ShapeDtypeStruct((1, mine, width), F32),
                jax.ShapeDtypeStruct((1, mine, width), F32),
            ),
            in_specs=[hbm, hbm, hbm, hbm, smem, smem, hbm],
            out_specs=(hbm, hbm, hbm),
            scratch_shapes=[
                pltpu.VMEM((tokens, width), BF16),
                pltpu.VMEM((tokens, width), BF16),
                pltpu.VMEM((tokens,), jnp.int32),
                pltpu.VMEM((2, block, 4 * width), BF16),
                pltpu.VMEM((2, 4, block, width), BF16),
                pltpu.VMEM((tokens, width), BF16),
                pltpu.VMEM((keys // LATENTS, tokens), F32),
                pltpu.VMEM((chunks, 2, 2, NX, part, cw), BF16),
                pltpu.VMEM((chunks, 2, NX, part, cw), BF16),
                pltpu.VMEM((chunks, 2, 2, part, cw), BF16),
                pltpu.VMEM((chunks, 2, 2, part, cw), BF16),
                pltpu.VMEM((chunks, 2, 2, 2, part, cw), BF16),
                pltpu.VMEM((chunks, GROUP, 2 * mine, cw), BF16),
                pltpu.VMEM((chunks, GROUP, 2 * mine, cw), BF16),
                pltpu.VMEM((mine, width), F32),
                pltpu.VMEM((mine, width), F32),
                dma((7,)),
                pltpu.SemaphoreType.REGULAR((4, 2)),
            ]
            + [dma((heads,))] * 6
            + [dma((chunks + 1,))] * 9
            + [dma((chunks + 1, 2))],
            compiler_params=pltpu.CompilerParams(
                collective_id=0, has_side_effects=True, vmem_limit_bytes=60 * 2**20
            ),
            name="attention_grads",
        )(
            queries, visual_keys, visual_values, out_grad, gate_value, image_order,
            image_seen,
        )
    )
    steps = 5
    return tuple(
        pl.pallas_call(
            hand_on,
            out_shape=tuple(jax.ShapeDtypeStruct(o.shape, o.dtype) for o in outs),
            in_specs=[hbm] * 3,
            out_specs=(hbm,) * 3,
            scratch_shapes=[
                pltpu.VMEM((steps, tokens // steps, width), BF16),
                pltpu.VMEM((2, mine, width), F32),
                dma((2, steps + 2)),
            ],
            compiler_params=pltpu.CompilerParams(vmem_limit_bytes=60 * 2**20),
            name="hand_on",
        )(*outs)
    )


def solution(mesh):
    placed = (
        P(None, "txt", "img"),
        P(None, "img", None),
        P(None, "img", None),
        P(None, "txt", "img"),
        P(None, "img"),
        P(),
        P("txt"),
    )
    return jax.shard_map(
        shards,
        mesh=mesh,
        in_specs=placed,
        out_specs=(P(None, "txt", "img"), P(None, "txt", "img"), P(None, "txt", "img")),
        check_vma=False,
    )
```

```python
import functools
import math
from typing import NamedTuple, Any

import jax
import jax.numpy as jnp
from jax import lax
from jax.experimental import pallas as pl
from jax.experimental.pallas import tpu as pltpu
from jax.sharding import PartitionSpec as P

MESH = pl.DeviceIdType.MESH
F32, BF16 = jnp.float32, jnp.bfloat16
HEAD = 128
LATENTS = 64
NX, NLO, NZ = 4, 2, 8
GROUP = NLO * NZ
PAIR, SECOND, THIRD = 2, 2, 4
PAIRED = (1, 5)
LAST_SECOND, LAST_THIRD = (9, 10), (11, 11)


class Unit(NamedTuple):
    chunk: Any
    cols: Any
    sem: Any
    whole: bool


def product(a, b, ca, cb):
    return lax.dot_general(a, b, (((ca,), (cb,)), ((), ())), preferred_element_type=F32)


def kernel(
    chunks, per, q_hbm, k_hbm, v_hbm, g_hbm, gate, order, seen_hbm, dq_hbm, kg_hbm, vg_hbm,
    q_s, g_s, seen_s, stage_s, kv_s, dq_s, may_s, part_s, pair_s, a_s, b_s, bc_s, zs_s, rz_s, kg_s, vg_s,
    own_sem, round_sem, cross_tx, cross_rx, mate_tx, mate_rx, relay_tx, relay_rx,
    pair_tx, pair_rx, first_tx, a_rx, b_tx, bc_rx, z_tx, z_rx, dq_sem, grad_sem,
):
    img, txt = lax.axis_index("img"), lax.axis_index("txt")
    hi, core = img // 2, lax.rem(img, 2)
    x, lo, z = txt // GROUP, lax.rem(txt // NZ, NLO), lax.rem(txt, NZ)
    slot = lax.rem(txt, GROUP)
    zq, zp = z // 2, lax.rem(z, 2)
    mine = zp * (GROUP // 2) + lo * (NZ // 2) + zq
    tokens, width = q_s.shape
    block = k_hbm.shape[1]
    half = block // 2
    keys = 4 * block
    images = keys // LATENTS
    cw = per * HEAD
    heads = chunks * per
    part = keys // (2 * NX)
    scale = 1.0 / math.sqrt(HEAD)
    scale2 = scale * math.log2(math.e)

    mate = (hi * 2 + 1 - core, txt)
    flipped = txt + (1 - 2 * lo) * NZ
    cross = [((1 - hi) * 2 + c, flipped) for c in range(2)]
    relay = (img, flipped)
    xp, xm, xo = lax.rem(x + 1, NX), lax.rem(x + NX - 1, NX), lax.rem(x + 2, NX)
    up, down = (img, xp * GROUP + slot), (img, xm * GROUP + slot)

    before, after = (img, txt - z + lax.rem(z + NZ - 1, NZ)), (img, txt - z + lax.rem(z + 1, NZ))

    def at_place(g):
        other = lax.rem(g // (NZ // 2), NLO) * NZ + lax.rem(g, NZ // 2) * 2 + g // (GROUP // 2)
        return (img, x * GROUP + other)

    def local(src, dst, sem):
        return pltpu.make_async_copy(src, dst, sem)

    def remote(src, dst, tx, rx, to):
        return pltpu.make_async_remote_copy(
            src_ref=src, dst_ref=dst, send_sem=tx, recv_sem=rx, device_id=to, device_id_type=MESH
        )

    def columns(c, base=0):
        return pl.ds(pl.multiple_of(base + c * cw, HEAD), cw)

    def rows(start, size):
        return pl.ds(pl.multiple_of(start, 16), size)

    barrier = pltpu.get_barrier_semaphore()
    near = [mate, *cross, relay, up, down, before, after]
    for to in near:
        pl.semaphore_signal(barrier, inc=1, device_id=to, device_id_type=MESH)
    own_columns = pl.ds(pl.multiple_of(img * width, HEAD), width)
    staged = [
        local(k_hbm.at[0], stage_s.at[0], own_sem.at[0]),
        local(v_hbm.at[0], stage_s.at[1], own_sem.at[1]),
    ]
    loads = [
        local(k_hbm.at[0, :, own_columns], kv_s.at[0, img], own_sem.at[2]),
        local(v_hbm.at[0, :, own_columns], kv_s.at[1, img], own_sem.at[3]),
        local(seen_hbm, seen_s, own_sem.at[4]),
        local(q_hbm.at[0], q_s, own_sem.at[5]),
        local(g_hbm.at[0], g_s, own_sem.at[6]),
    ]
    for copy in staged + loads:
        copy.start()
    for copy in staged:
        copy.wait()
    pl.semaphore_wait(barrier, len(near))

    def tell(r):
        pl.semaphore_signal(round_sem.at[r, 0], inc=1, device_id=after, device_id_type=MESH)
        pl.semaphore_signal(round_sem.at[r, 1], inc=1, device_id=before, device_id_type=MESH)

    def hear(r):
        pl.semaphore_wait(round_sem.at[r, 0], 1)
        pl.semaphore_wait(round_sem.at[r, 1], 1)

    tell(0)

    def one_head(h, base=0):
        return pl.ds(pl.multiple_of(base + h * HEAD, HEAD), HEAD)

    def cross_piece(h):
        return kv_s.at[:, pl.ds(2 * (1 - hi), 2), rows(lo * half, half), one_head(h)]

    def relay_piece(h):
        return kv_s.at[:, pl.ds(2 * (1 - hi), 2), rows((1 - lo) * half, half), one_head(h)]

    def mate_piece(h):
        return kv_s.at[:, hi * 2 + 1 - core, :, one_head(h)]

    def cross_send(h, to):
        sent = rows((1 - lo) * half, half)
        return remote(
            stage_s.at[:, sent, one_head(h, to[0] * width)], kv_s.at[:, img, sent, one_head(h)],
            cross_tx.at[h], cross_rx.at[h], to,
        )

    def mate_send(h):
        return remote(
            stage_s.at[:, :, one_head(h, mate[0] * width)], kv_s.at[:, img, :, one_head(h)],
            mate_tx.at[h], mate_rx.at[h], mate,
        )

    def send_latents(h, carry):
        for to in cross:
            cross_send(h, to).start()
        mate_send(h).start()
        return carry

    lax.fori_loop(0, heads, send_latents, 0)
    hear(0)
    tell(1)
    for copy in loads:
        copy.wait()
    may_s[...] = jnp.concatenate(
        [jnp.where(order[0, b] < seen_s[...].reshape(1, tokens), 1.0, 0.0) for b in range(images)],
        axis=0,
    )

    def pass_on(h):
        piece = cross_piece(h)
        remote(piece, piece, cross_tx.at[h], cross_rx.at[h], relay).wait_recv()
        remote(piece, piece, relay_tx.at[h], relay_rx.at[h], relay).start()

    def latents_ready(h):
        piece = mate_piece(h)
        remote(piece, piece, mate_tx.at[h], mate_rx.at[h], mate).wait_recv()

        piece = relay_piece(h)
        remote(piece, piece, relay_tx.at[h], relay_rx.at[h], relay).wait_recv()

    def keep(c, a, at, value):
        by_parity = value.reshape(keys // 16, 2, 8, HEAD)
        for p in range(2):
            rows_p = by_parity[:, p].reshape(NX, part, HEAD)
            part_s[c, p, a, :, :, at] = rows_p.astype(BF16)

    def head(c, j):
        h = c * per + j
        cols = pl.ds(pl.multiple_of(h * HEAD, HEAD), HEAD)
        k = kv_s[0, :, :, cols].reshape(keys, HEAD)
        v = kv_s[1, :, :, cols].reshape(keys, HEAD)
        q = q_s[:, cols]
        factor = jnp.tanh(jnp.full((8, HEAD), gate[0, h], F32))[0:1]
        gated = (g_s[:, cols].astype(F32) * factor).astype(BF16)
        may = may_s[...] > 0
        scores = product(k, q, 1, 1).reshape(images, LATENTS, tokens)
        top = jnp.where(may, jnp.max(scores, axis=1), -1e30)
        top = jnp.max(top, axis=0, keepdims=True)
        off = jnp.where(may, top, 1e30)
        exponent = jnp.exp2((scores - off[:, None, :]) * scale2).reshape(keys, tokens)
        weights = exponent * (1.0 / jnp.sum(exponent, axis=0, keepdims=True))
        weight_grad = product(v, gated, 1, 1)
        delta = jnp.sum(weights * weight_grad, axis=0, keepdims=True)
        score_half = (weights * (weight_grad - delta)).astype(BF16)
        weight_half = weights.astype(BF16)
        at = pl.ds(j * HEAD, HEAD)
        keep(c, 1, at, product(weight_half, gated, 1, 0))
        keep(c, 0, at, product(score_half, q, 1, 0) * scale)
        dq_s[:, cols] = (product(score_half, k, 0, 0) * scale).astype(BF16)

    def dq_copy(c):
        return local(dq_s.at[:, columns(c)], dq_hbm.at[0, :, columns(c)], dq_sem.at[c])

    def pair_of(c):
        odd = lax.rem(c // 2, 2)
        return jnp.where(zp == odd, 1, -1)

    def pair_send(u):
        c = u.chunk
        to = (img, txt - z + lax.rem(z + NZ + pair_of(c), NZ))
        return remote(part_s.at[c, 1 - zp], pair_s.at[c], pair_tx.at[c], pair_rx.at[c], to)

    def pair_sum(u):
        c = u.chunk
        pair_send(u).wait_recv()
        for a in range(2):
            for i in range(NX):
                both = part_s[c, zp, a, i].astype(F32) + pair_s[c, a, i].astype(F32)
                part_s[c, zp, a, i] = both.astype(BF16)

    def parities(u):
        return pl.ds(0, 2) if u.whole else pl.ds(0, 1)

    def slab_of(u, a, i):
        return part_s.at[u.chunk, pl.ds(0, 2) if u.whole else pl.ds(zp, 1), a, i, :, u.cols]

    def a_of(u, a):
        return a_s.at[u.chunk, a, parities(u), :, u.cols]

    def b_of(u, a):
        return b_s.at[u.chunk, a, parities(u), :, u.cols]

    def bc_of(u, hop, a):
        return bc_s.at[u.chunk, hop, a, parities(u), :, u.cols]

    both_arrays = pl.ds(0, 2)

    def first_sends(u):
        tx, rx_a, rx_c = first_tx.at[u.sem], a_rx.at[u.sem], bc_rx.at[u.sem]
        return [
            remote(slab_of(u, 0, xo), a_of(u, 0), tx, rx_a, down),
            remote(slab_of(u, 1, xo), a_of(u, 1), tx, rx_a, up),
            remote(slab_of(u, 0, xp), bc_of(u, 1, 0), tx, rx_c, up),
            remote(slab_of(u, 1, xm), bc_of(u, 1, 1), tx, rx_c, down),
        ]

    def second_sends(u):
        return [
            remote(b_of(u, a), bc_of(u, 0, a), b_tx.at[u.sem], bc_rx.at[u.sem], to)
            for a, to in enumerate((down, up))
        ]

    def second_hop(u):
        piece = a_of(u, both_arrays)
        remote(piece, piece, first_tx.at[u.sem], a_rx.at[u.sem], down).wait_recv()
        for a, i in enumerate((xm, xp)):
            for p in range(2 if u.whole else 1):
                own = part_s[u.chunk, p if u.whole else zp, a, i, :, u.cols].astype(F32)
                total = a_s[u.chunk, a, p, :, u.cols].astype(F32) + own
                b_s[u.chunk, a, p, :, u.cols] = total.astype(BF16)

    def x_sum(u):
        piece = bc_of(u, pl.ds(0, 2), both_arrays)
        remote(piece, piece, b_tx.at[u.sem], bc_rx.at[u.sem], down).wait_recv()
        c = u.chunk
        for p in range(2 if u.whole else 1):
            parity = p if u.whole else zp
            both = [
                (
                    part_s[c, parity, a, x, :, u.cols].astype(F32)
                    + bc_s[c, 0, a, p, :, u.cols].astype(F32)
                    + bc_s[c, 1, a, p, :, u.cols].astype(F32)
                ).reshape(GROUP // 2, 8, u.cols.size)
                for a in range(2)
            ]
            places = pl.ds(parity * (GROUP // 2), GROUP // 2)
            zs_s[c, places, :, u.cols] = jnp.concatenate(both, axis=1).astype(BF16)
        rz_s[c, mine, :, u.cols] = zs_s[c, mine, :, u.cols]

    def spread(u):
        size = GROUP if u.whole else GROUP // 2

        def one(j, carry):
            if u.whole:
                g = lax.rem(mine + j, GROUP)
            else:
                g = zp * size + lax.rem(mine + j, size)
            remote(
                zs_s.at[u.chunk, g, :, u.cols], rz_s.at[u.chunk, mine, :, u.cols],
                z_tx.at[u.sem], z_rx.at[u.sem], at_place(g),
            ).start()
            return carry

        lax.fori_loop(1, size, one, 0)

    def others(ref, u):
        return ref.at[u.chunk, pl.ds(0, (GROUP if u.whole else GROUP // 2) - 1), :, u.cols]

    def finish(u):
        piece = others(rz_s, u)
        remote(piece, piece, z_tx.at[u.sem], z_rx.at[u.sem], relay).wait_recv()
        places = pl.ds(0, GROUP) if u.whole else pl.ds(zp * (GROUP // 2), GROUP // 2)
        total = jnp.sum(rz_s[u.chunk, places, :, u.cols].astype(F32), axis=0)
        at = grad_columns(u)
        kg_s[:, at] = total[:8]
        vg_s[:, at] = total[8:]
        for copy in grad_copies(at, u.sem):
            copy.start()

    def grad_columns(u):
        if isinstance(u.chunk, int):
            return pl.ds(u.chunk * cw + u.cols.start, u.cols.size)
        return columns(u.chunk)

    def grad_copies(at, sem):
        return [
            local(kg_s.at[:, at], kg_hbm.at[0, :, at], grad_sem.at[sem, 0]),
            local(vg_s.at[:, at], vg_hbm.at[0, :, at], grad_sem.at[sem, 1]),
        ]

    def start(copies):
        for copy in copies:
            copy.start()

    def after_compute(u):
        if u.whole:
            start(first_sends(u))
        else:
            pair_send(u).start()

    def first_stage(u):
        pair_sum(u)
        start(first_sends(u))

    def second_stage(u):
        second_hop(u)
        start(second_sends(u))

    def third_stage(u):
        x_sum(u)
        spread(u)

    def unit(c, whole):
        return Unit(c, pl.ds(0, cw), c, whole)

    last = chunks - 1
    ends = [Unit(last, pl.ds(j * HEAD, HEAD), last + j, True) for j in range(per)]

    def paired(c):
        return functools.reduce(lambda t, d: t | (c == d), PAIRED, c < 0)

    def each(c, act, forms=(True, False)):
        for whole in forms:
            fits = (c >= 0) & (c < last) & (paired(c) != whole)
            pl.when(fits)(functools.partial(act, unit(c, whole)))

    def compute(h, c, j):
        @pl.when(h + 2 < heads)
        def _():
            pass_on(h + 2)

        latents_ready(h)
        head(c, j)

    hear(1)
    tell(2)
    pass_on(0)
    hear(2)
    tell(3)
    pass_on(1)

    def step(s, carry):
        def one(j, inner):
            compute(s * per + j, s, j)
            return inner

        lax.fori_loop(0, per, one, 0)
        dq_copy(s).start()
        each(s, after_compute)
        pl.when(s == 0)(lambda: hear(3))
        each(s - PAIR, first_stage, (False,))
        each(s - SECOND, second_stage, (True,))
        each(s - PAIR - SECOND, second_stage, (False,))
        each(s - THIRD, third_stage, (True,))
        each(s - PAIR - THIRD, third_stage, (False,))
        return carry

    lax.fori_loop(0, last, step, 0)
    for j, u in enumerate(ends):
        compute(last * per + j, last, j)
        after_compute(u)

    dq_copy(last).start()

    due = {}
    for c in range(last):
        late = PAIR if c in PAIRED else 0
        for at, act in ((0, first_stage), (SECOND, second_stage), (THIRD, third_stage)):
            if c + late + at >= last and (at or late):
                due.setdefault(c + late + at, []).append((act, unit(c, c not in PAIRED)))
    for u, second, third in zip(ends, LAST_SECOND, LAST_THIRD):
        due.setdefault(second, []).append((second_stage, u))
        due.setdefault(third, []).append((third_stage, u))
    def settle_head(h, carry):
        piece = cross_piece(h)
        remote(piece, piece, cross_tx.at[h], cross_rx.at[h], relay).wait_send()
        remote(piece, piece, relay_tx.at[h], relay_rx.at[h], relay).wait_send()
        mate_send(h).wait_send()
        return carry

    def settle_unit(u):
        if not u.whole:
            pair_send(u).wait_send()
        piece = bc_of(u, pl.ds(0, 2), both_arrays)
        remote(piece, piece, first_tx.at[u.sem], bc_rx.at[u.sem], down).wait_send()
        piece = b_of(u, both_arrays)
        remote(piece, piece, b_tx.at[u.sem], bc_rx.at[u.sem], down).wait_send()
        piece = others(zs_s, u)
        remote(piece, piece, z_tx.at[u.sem], z_rx.at[u.sem], relay).wait_send()

    def settle_grads(u):
        for copy in grad_copies(grad_columns(u), u.sem):
            copy.wait()

    def settle(c, carry):
        dq_copy(c).wait()
        each(c, settle_unit)
        return carry

    def settle_all_grads(c, carry):
        each(c, settle_grads)
        return carry

    for s in sorted(due):
        for act, u in due[s]:
            act(u)
        if s == last:
            lax.fori_loop(0, heads, settle_head, 0)

    def end(c, carry):
        each(c, finish)
        return carry

    lax.fori_loop(0, last - 1, settle, 0)
    lax.fori_loop(0, last, end, 0)
    for u in ends:
        finish(u)
    lax.fori_loop(last - 1, chunks, settle, 0)
    lax.fori_loop(0, last, settle_all_grads, 0)
    for u in ends:
        settle_unit(u)
        settle_grads(u)


def hand_on(dq_in, kg_in, vg_in, dq_out, kg_out, vg_out, dq_s, grad_s, sem):
    steps = dq_s.shape[0]
    rows = dq_s.shape[1]
    pairs = [
        (dq_in.at[0, pl.ds(i * rows, rows)], dq_s.at[i], dq_out.at[0, pl.ds(i * rows, rows)])
        for i in range(steps)
    ]
    pairs += [(kg_in.at[0], grad_s.at[0], kg_out.at[0]), (vg_in.at[0], grad_s.at[1], vg_out.at[0])]
    loads = [pltpu.make_async_copy(a, b, sem.at[0, i]) for i, (a, b, _) in enumerate(pairs)]
    stores = [pltpu.make_async_copy(b, c, sem.at[1, i]) for i, (_, b, c) in enumerate(pairs)]
    for copy in loads:
        copy.start()
    for load, store in zip(loads, stores):
        load.wait()
        store.start()
    for copy in stores:
        copy.wait()


def shards(queries, visual_keys, visual_values, out_grad, gate_value, image_order, image_seen):
    _, tokens, width = queries.shape
    block = visual_keys.shape[1]
    keys = 4 * block
    heads = width // HEAD
    per = 2
    chunks = heads // per
    cw = per * HEAD
    part = keys // (2 * NX)
    mine = keys // (NX * GROUP)
    hbm = pl.BlockSpec(memory_space=pl.ANY)
    smem = pl.BlockSpec(memory_space=pltpu.SMEM)
    dma = pltpu.SemaphoreType.DMA
    outs = tuple(
        pl.pallas_call(
            functools.partial(kernel, chunks, per),
            out_shape=(
                jax.ShapeDtypeStruct((1, tokens, width), BF16),
                jax.ShapeDtypeStruct((1, mine, width), F32),
                jax.ShapeDtypeStruct((1, mine, width), F32),
            ),
            in_specs=[hbm, hbm, hbm, hbm, smem, smem, hbm],
            out_specs=(hbm, hbm, hbm),
            scratch_shapes=[
                pltpu.VMEM((tokens, width), BF16),
                pltpu.VMEM((tokens, width), BF16),
                pltpu.VMEM((tokens,), jnp.int32),
                pltpu.VMEM((2, block, 4 * width), BF16),
                pltpu.VMEM((2, 4, block, width), BF16),
                pltpu.VMEM((tokens, width), BF16),
                pltpu.VMEM((keys // LATENTS, tokens), F32),
                pltpu.VMEM((chunks, 2, 2, NX, part, cw), BF16),
                pltpu.VMEM((chunks, 2, NX, part, cw), BF16),
                pltpu.VMEM((chunks, 2, 2, part, cw), BF16),
                pltpu.VMEM((chunks, 2, 2, part, cw), BF16),
                pltpu.VMEM((chunks, 2, 2, 2, part, cw), BF16),
                pltpu.VMEM((chunks, GROUP, 2 * mine, cw), BF16),
                pltpu.VMEM((chunks, GROUP, 2 * mine, cw), BF16),
                pltpu.VMEM((mine, width), F32),
                pltpu.VMEM((mine, width), F32),
                dma((7,)),
                pltpu.SemaphoreType.REGULAR((4, 2)),
            ]
            + [dma((heads,))] * 6
            + [dma((chunks + 1,))] * 9
            + [dma((chunks + 1, 2))],
            compiler_params=pltpu.CompilerParams(
                collective_id=0, has_side_effects=True, vmem_limit_bytes=60 * 2**20
            ),
            name="attention_grads",
        )(
            queries, visual_keys, visual_values, out_grad, gate_value, image_order,
            image_seen,
        )
    )
    steps = 5
    return tuple(
        pl.pallas_call(
            hand_on,
            out_shape=tuple(jax.ShapeDtypeStruct(o.shape, o.dtype) for o in outs),
            in_specs=[hbm] * 3,
            out_specs=(hbm,) * 3,
            scratch_shapes=[
                pltpu.VMEM((steps, tokens // steps, width), BF16),
                pltpu.VMEM((2, mine, width), F32),
                dma((2, steps + 2)),
            ],
            compiler_params=pltpu.CompilerParams(vmem_limit_bytes=60 * 2**20),
            name="hand_on",
        )(*outs)
    )


def solution(mesh):
    placed = (
        P(None, "txt", "img"),
        P(None, "img", None),
        P(None, "img", None),
        P(None, "txt", "img"),
        P(None, "img"),
        P(),
        P("txt"),
    )
    return jax.shard_map(
        shards,
        mesh=mesh,
        in_specs=placed,
        out_specs=(P(None, "txt", "img"), P(None, "txt", "img"), P(None, "txt", "img")),
        check_vma=False,
    )
```

```python
import functools
import math
from typing import NamedTuple, Any

import jax
import jax.numpy as jnp
from jax import lax
from jax.experimental import pallas as pl
from jax.experimental.pallas import tpu as pltpu
from jax.sharding import PartitionSpec as P

MESH = pl.DeviceIdType.MESH
F32, BF16 = jnp.float32, jnp.bfloat16
HEAD = 128
LATENTS = 64
NX, NLO, NZ = 4, 2, 8
GROUP = NLO * NZ
PAIR, SECOND, THIRD = 2, 2, 4
PAIRED = (1, 5)
LAST_SECOND, LAST_THIRD = (9, 10), (11, 11)


class Unit(NamedTuple):
    chunk: Any
    cols: Any
    sem: Any
    whole: bool


def product(a, b, ca, cb):
    return lax.dot_general(a, b, (((ca,), (cb,)), ((), ())), preferred_element_type=F32)


def kernel(
    chunks, per, q_hbm, k_hbm, v_hbm, g_hbm, gate, order, seen_hbm, dq_hbm, kg_hbm, vg_hbm,
    q_s, g_s, seen_s, stage_s, kv_s, dq_s, may_s, part_s, pair_s, a_s, b_s, bc_s, zs_s, rz_s, kg_s, vg_s,
    own_sem, round_sem, cross_tx, cross_rx, mate_tx, mate_rx, relay_tx, relay_rx,
    pair_tx, pair_rx, first_tx, a_rx, b_tx, bc_rx, z_tx, z_rx, dq_sem, grad_sem,
):
    img, txt = lax.axis_index("img"), lax.axis_index("txt")
    hi, core = img // 2, lax.rem(img, 2)
    x, lo, z = txt // GROUP, lax.rem(txt // NZ, NLO), lax.rem(txt, NZ)
    slot = lax.rem(txt, GROUP)
    zq, zp = z // 2, lax.rem(z, 2)
    mine = zp * (GROUP // 2) + lo * (NZ // 2) + zq
    tokens, width = q_s.shape
    block = k_hbm.shape[1]
    half = block // 2
    keys = 4 * block
    images = keys // LATENTS
    cw = per * HEAD
    heads = chunks * per
    part = keys // (2 * NX)
    scale = 1.0 / math.sqrt(HEAD)
    scale2 = scale * math.log2(math.e)

    mate = (hi * 2 + 1 - core, txt)
    flipped = txt + (1 - 2 * lo) * NZ
    cross = [((1 - hi) * 2 + c, flipped) for c in range(2)]
    relay = (img, flipped)
    xp, xm, xo = lax.rem(x + 1, NX), lax.rem(x + NX - 1, NX), lax.rem(x + 2, NX)
    up, down = (img, xp * GROUP + slot), (img, xm * GROUP + slot)

    before, after = (img, txt - z + lax.rem(z + NZ - 1, NZ)), (img, txt - z + lax.rem(z + 1, NZ))

    def at_place(g):
        other = lax.rem(g // (NZ // 2), NLO) * NZ + lax.rem(g, NZ // 2) * 2 + g // (GROUP // 2)
        return (img, x * GROUP + other)

    def local(src, dst, sem):
        return pltpu.make_async_copy(src, dst, sem)

    def remote(src, dst, tx, rx, to):
        return pltpu.make_async_remote_copy(
            src_ref=src, dst_ref=dst, send_sem=tx, recv_sem=rx, device_id=to, device_id_type=MESH
        )

    def columns(c, base=0):
        return pl.ds(pl.multiple_of(base + c * cw, HEAD), cw)

    def rows(start, size):
        return pl.ds(pl.multiple_of(start, 16), size)

    barrier = pltpu.get_barrier_semaphore()
    near = [mate, *cross, relay, up, down, before, after]
    for to in near:
        pl.semaphore_signal(barrier, inc=1, device_id=to, device_id_type=MESH)
    own_columns = pl.ds(pl.multiple_of(img * width, HEAD), width)
    staged = [
        local(k_hbm.at[0], stage_s.at[0], own_sem.at[0]),
        local(v_hbm.at[0], stage_s.at[1], own_sem.at[1]),
    ]
    loads = [
        local(k_hbm.at[0, :, own_columns], kv_s.at[0, img], own_sem.at[2]),
        local(v_hbm.at[0, :, own_columns], kv_s.at[1, img], own_sem.at[3]),
        local(seen_hbm, seen_s, own_sem.at[4]),
        local(q_hbm.at[0], q_s, own_sem.at[5]),
        local(g_hbm.at[0], g_s, own_sem.at[6]),
    ]
    for copy in staged + loads:
        copy.start()
    for copy in staged:
        copy.wait()
    pl.semaphore_wait(barrier, len(near))

    def tell(r):
        pl.semaphore_signal(round_sem.at[r, 0], inc=1, device_id=after, device_id_type=MESH)
        pl.semaphore_signal(round_sem.at[r, 1], inc=1, device_id=before, device_id_type=MESH)

    def hear(r):
        pl.semaphore_wait(round_sem.at[r, 0], 1)
        pl.semaphore_wait(round_sem.at[r, 1], 1)

    tell(0)

    def one_head(h, base=0):
        return pl.ds(pl.multiple_of(base + h * HEAD, HEAD), HEAD)

    def cross_piece(h):
        return kv_s.at[:, pl.ds(2 * (1 - hi), 2), rows(lo * half, half), one_head(h)]

    def relay_piece(h):
        return kv_s.at[:, pl.ds(2 * (1 - hi), 2), rows((1 - lo) * half, half), one_head(h)]

    def mate_piece(h):
        return kv_s.at[:, hi * 2 + 1 - core, :, one_head(h)]

    def cross_send(h, to):
        sent = rows((1 - lo) * half, half)
        return remote(
            stage_s.at[:, sent, one_head(h, to[0] * width)], kv_s.at[:, img, sent, one_head(h)],
            cross_tx.at[h], cross_rx.at[h], to,
        )

    def mate_send(h):
        return remote(
            stage_s.at[:, :, one_head(h, mate[0] * width)], kv_s.at[:, img, :, one_head(h)],
            mate_tx.at[h], mate_rx.at[h], mate,
        )

    def send_latents(h, carry):
        for to in cross:
            cross_send(h, to).start()
        mate_send(h).start()
        return carry

    lax.fori_loop(0, heads, send_latents, 0)
    hear(0)
    tell(1)
    for copy in loads:
        copy.wait()
    may_s[...] = jnp.concatenate(
        [jnp.where(order[0, b] < seen_s[...].reshape(1, tokens), 1.0, 0.0) for b in range(images)],
        axis=0,
    )

    def pass_on(h):
        piece = cross_piece(h)
        remote(piece, piece, cross_tx.at[h], cross_rx.at[h], relay).wait_recv()
        remote(piece, piece, relay_tx.at[h], relay_rx.at[h], relay).start()

    def latents_ready(h):
        piece = mate_piece(h)
        remote(piece, piece, mate_tx.at[h], mate_rx.at[h], mate).wait_recv()

        piece = relay_piece(h)
        remote(piece, piece, relay_tx.at[h], relay_rx.at[h], relay).wait_recv()

    def keep(c, a, at, value):
        by_parity = value.reshape(keys // 16, 2, 8, HEAD)
        for p in range(2):
            rows_p = by_parity[:, p].reshape(NX, part, HEAD)
            part_s[c, p, a, :, :, at] = rows_p.astype(BF16)

    def head(c, j):
        h = c * per + j
        cols = pl.ds(pl.multiple_of(h * HEAD, HEAD), HEAD)
        k = kv_s[0, :, :, cols].reshape(keys, HEAD)
        v = kv_s[1, :, :, cols].reshape(keys, HEAD)
        q = q_s[:, cols]
        factor = jnp.tanh(jnp.full((8, HEAD), gate[0, h], F32))[0:1]
        gated = (g_s[:, cols].astype(F32) * factor).astype(BF16)
        may = may_s[...] > 0
        scores = product(k, q, 1, 1).reshape(images, LATENTS, tokens)
        top = jnp.where(may, jnp.max(scores, axis=1), -1e30)
        top = jnp.max(top, axis=0, keepdims=True)
        off = jnp.where(may, top, 1e30)
        exponent = jnp.exp2((scores - off[:, None, :]) * scale2).reshape(keys, tokens)
        weights = exponent * (1.0 / jnp.sum(exponent, axis=0, keepdims=True))
        weight_grad = product(v, gated, 1, 1)
        delta = jnp.sum(weights * weight_grad, axis=0, keepdims=True)
        score_half = (weights * (weight_grad - delta)).astype(BF16)
        weight_half = weights.astype(BF16)
        at = pl.ds(j * HEAD, HEAD)
        keep(c, 1, at, product(weight_half, gated, 1, 0))
        keep(c, 0, at, product(score_half, q, 1, 0) * scale)
        dq_s[:, cols] = (product(score_half, k, 0, 0) * scale).astype(BF16)

    def dq_copy(c):
        return local(dq_s.at[:, columns(c)], dq_hbm.at[0, :, columns(c)], dq_sem.at[c])

    def pair_of(c):
        odd = lax.rem(c // 2, 2)
        return jnp.where(zp == odd, 1, -1)

    def pair_send(u):
        c = u.chunk
        to = (img, txt - z + lax.rem(z + NZ + pair_of(c), NZ))
        return remote(part_s.at[c, 1 - zp], pair_s.at[c], pair_tx.at[c], pair_rx.at[c], to)

    def pair_sum(u):
        c = u.chunk
        pair_send(u).wait_recv()
        for a in range(2):
            for i in range(NX):
                both = part_s[c, zp, a, i].astype(F32) + pair_s[c, a, i].astype(F32)
                part_s[c, zp, a, i] = both.astype(BF16)

    def parities(u):
        return pl.ds(0, 2) if u.whole else pl.ds(0, 1)

    def slab_of(u, a, i):
        return part_s.at[u.chunk, pl.ds(0, 2) if u.whole else pl.ds(zp, 1), a, i, :, u.cols]

    def a_of(u, a):
        return a_s.at[u.chunk, a, parities(u), :, u.cols]

    def b_of(u, a):
        return b_s.at[u.chunk, a, parities(u), :, u.cols]

    def bc_of(u, hop, a):
        return bc_s.at[u.chunk, hop, a, parities(u), :, u.cols]

    both_arrays = pl.ds(0, 2)

    def first_sends(u):
        tx, rx_a, rx_c = first_tx.at[u.sem], a_rx.at[u.sem], bc_rx.at[u.sem]
        return [
            remote(slab_of(u, 0, xo), a_of(u, 0), tx, rx_a, down),
            remote(slab_of(u, 1, xo), a_of(u, 1), tx, rx_a, up),
            remote(slab_of(u, 0, xp), bc_of(u, 1, 0), tx, rx_c, up),
            remote(slab_of(u, 1, xm), bc_of(u, 1, 1), tx, rx_c, down),
        ]

    def second_sends(u):
        return [
            remote(b_of(u, a), bc_of(u, 0, a), b_tx.at[u.sem], bc_rx.at[u.sem], to)
            for a, to in enumerate((down, up))
        ]

    def second_hop(u):
        piece = a_of(u, both_arrays)
        remote(piece, piece, first_tx.at[u.sem], a_rx.at[u.sem], down).wait_recv()
        for a, i in enumerate((xm, xp)):
            for p in range(2 if u.whole else 1):
                own = part_s[u.chunk, p if u.whole else zp, a, i, :, u.cols].astype(F32)
                total = a_s[u.chunk, a, p, :, u.cols].astype(F32) + own
                b_s[u.chunk, a, p, :, u.cols] = total.astype(BF16)

    def x_sum(u):
        piece = bc_of(u, pl.ds(0, 2), both_arrays)
        remote(piece, piece, b_tx.at[u.sem], bc_rx.at[u.sem], down).wait_recv()
        c = u.chunk
        for p in range(2 if u.whole else 1):
            parity = p if u.whole else zp
            both = [
                (
                    part_s[c, parity, a, x, :, u.cols].astype(F32)
                    + bc_s[c, 0, a, p, :, u.cols].astype(F32)
                    + bc_s[c, 1, a, p, :, u.cols].astype(F32)
                ).reshape(GROUP // 2, 8, u.cols.size)
                for a in range(2)
            ]
            places = pl.ds(parity * (GROUP // 2), GROUP // 2)
            zs_s[c, places, :, u.cols] = jnp.concatenate(both, axis=1).astype(BF16)
        rz_s[c, mine, :, u.cols] = zs_s[c, mine, :, u.cols]

    def spread(u):
        size = GROUP if u.whole else GROUP // 2

        stride = 1 if u.whole else 2

        def one(t, carry):
            m = t // 2
            dz = NZ // 2 + stride * ((m + 1) // 2) * (1 - 2 * lax.rem(m, 2))
            y, zz = lax.rem(lo + 1 + t, NLO), lax.rem(z + dz, NZ)
            g = lax.rem(zz, 2) * (GROUP // 2) + y * (NZ // 2) + zz // 2
            remote(
                zs_s.at[u.chunk, g, :, u.cols], rz_s.at[u.chunk, mine, :, u.cols],
                z_tx.at[u.sem], z_rx.at[u.sem], at_place(g),
            ).start()
            return carry

        lax.fori_loop(0, size - 1, one, 0)

    def others(ref, u):
        return ref.at[u.chunk, pl.ds(0, (GROUP if u.whole else GROUP // 2) - 1), :, u.cols]

    def finish(u):
        piece = others(rz_s, u)
        remote(piece, piece, z_tx.at[u.sem], z_rx.at[u.sem], relay).wait_recv()
        places = pl.ds(0, GROUP) if u.whole else pl.ds(zp * (GROUP // 2), GROUP // 2)
        total = jnp.sum(rz_s[u.chunk, places, :, u.cols].astype(F32), axis=0)
        at = grad_columns(u)
        kg_s[:, at] = total[:8]
        vg_s[:, at] = total[8:]
        for copy in grad_copies(at, u.sem):
            copy.start()

    def grad_columns(u):
        if isinstance(u.chunk, int):
            return pl.ds(u.chunk * cw + u.cols.start, u.cols.size)
        return columns(u.chunk)

    def grad_copies(at, sem):
        return [
            local(kg_s.at[:, at], kg_hbm.at[0, :, at], grad_sem.at[sem, 0]),
            local(vg_s.at[:, at], vg_hbm.at[0, :, at], grad_sem.at[sem, 1]),
        ]

    def start(copies):
        for copy in copies:
            copy.start()

    def after_compute(u):
        if u.whole:
            start(first_sends(u))
        else:
            pair_send(u).start()

    def first_stage(u):
        pair_sum(u)
        start(first_sends(u))

    def second_stage(u):
        second_hop(u)
        start(second_sends(u))

    def third_stage(u):
        x_sum(u)
        spread(u)

    def unit(c, whole):
        return Unit(c, pl.ds(0, cw), c, whole)

    last = chunks - 1
    ends = [Unit(last, pl.ds(j * HEAD, HEAD), last + j, True) for j in range(per)]

    def paired(c):
        return functools.reduce(lambda t, d: t | (c == d), PAIRED, c < 0)

    def each(c, act, forms=(True, False)):
        for whole in forms:
            fits = (c >= 0) & (c < last) & (paired(c) != whole)
            pl.when(fits)(functools.partial(act, unit(c, whole)))

    def compute(h, c, j):
        @pl.when(h + 2 < heads)
        def _():
            pass_on(h + 2)

        latents_ready(h)
        head(c, j)

    hear(1)
    tell(2)
    pass_on(0)
    hear(2)
    tell(3)
    pass_on(1)

    def step(s, carry):
        def one(j, inner):
            compute(s * per + j, s, j)
            return inner

        lax.fori_loop(0, per, one, 0)
        dq_copy(s).start()
        each(s, after_compute)
        pl.when(s == 0)(lambda: hear(3))
        each(s - PAIR, first_stage, (False,))
        each(s - SECOND, second_stage, (True,))
        each(s - PAIR - SECOND, second_stage, (False,))
        each(s - THIRD, third_stage, (True,))
        each(s - PAIR - THIRD, third_stage, (False,))
        return carry

    lax.fori_loop(0, last, step, 0)
    for j, u in enumerate(ends):
        compute(last * per + j, last, j)
        after_compute(u)

    dq_copy(last).start()

    due = {}
    for c in range(last):
        late = PAIR if c in PAIRED else 0
        for at, act in ((0, first_stage), (SECOND, second_stage), (THIRD, third_stage)):
            if c + late + at >= last and (at or late):
                due.setdefault(c + late + at, []).append((act, unit(c, c not in PAIRED)))
    for u, second, third in zip(ends, LAST_SECOND, LAST_THIRD):
        due.setdefault(second, []).append((second_stage, u))
        due.setdefault(third, []).append((third_stage, u))
    def settle_head(h, carry):
        piece = cross_piece(h)
        remote(piece, piece, cross_tx.at[h], cross_rx.at[h], relay).wait_send()
        remote(piece, piece, relay_tx.at[h], relay_rx.at[h], relay).wait_send()
        mate_send(h).wait_send()
        return carry

    def settle_unit(u):
        if not u.whole:
            pair_send(u).wait_send()
        piece = bc_of(u, pl.ds(0, 2), both_arrays)
        remote(piece, piece, first_tx.at[u.sem], bc_rx.at[u.sem], down).wait_send()
        piece = b_of(u, both_arrays)
        remote(piece, piece, b_tx.at[u.sem], bc_rx.at[u.sem], down).wait_send()
        piece = others(zs_s, u)
        remote(piece, piece, z_tx.at[u.sem], z_rx.at[u.sem], relay).wait_send()

    def settle_grads(u):
        for copy in grad_copies(grad_columns(u), u.sem):
            copy.wait()

    def settle(c, carry):
        dq_copy(c).wait()
        each(c, settle_unit)
        return carry

    def settle_all_grads(c, carry):
        each(c, settle_grads)
        return carry

    for s in sorted(due):
        for act, u in due[s]:
            act(u)
        if s == last:
            lax.fori_loop(0, heads, settle_head, 0)

    def end(c, carry):
        each(c, finish)
        return carry

    lax.fori_loop(0, last - 1, settle, 0)
    lax.fori_loop(0, last, end, 0)
    for u in ends:
        finish(u)
    lax.fori_loop(last - 1, chunks, settle, 0)
    lax.fori_loop(0, last, settle_all_grads, 0)
    for u in ends:
        settle_unit(u)
        settle_grads(u)


def hand_on(dq_in, kg_in, vg_in, dq_out, kg_out, vg_out, dq_s, grad_s, sem):
    steps = dq_s.shape[0]
    rows = dq_s.shape[1]
    pairs = [
        (dq_in.at[0, pl.ds(i * rows, rows)], dq_s.at[i], dq_out.at[0, pl.ds(i * rows, rows)])
        for i in range(steps)
    ]
    pairs += [(kg_in.at[0], grad_s.at[0], kg_out.at[0]), (vg_in.at[0], grad_s.at[1], vg_out.at[0])]
    loads = [pltpu.make_async_copy(a, b, sem.at[0, i]) for i, (a, b, _) in enumerate(pairs)]
    stores = [pltpu.make_async_copy(b, c, sem.at[1, i]) for i, (_, b, c) in enumerate(pairs)]
    for copy in loads:
        copy.start()
    for load, store in zip(loads, stores):
        load.wait()
        store.start()
    for copy in stores:
        copy.wait()


def shards(queries, visual_keys, visual_values, out_grad, gate_value, image_order, image_seen):
    _, tokens, width = queries.shape
    block = visual_keys.shape[1]
    keys = 4 * block
    heads = width // HEAD
    per = 2
    chunks = heads // per
    cw = per * HEAD
    part = keys // (2 * NX)
    mine = keys // (NX * GROUP)
    hbm = pl.BlockSpec(memory_space=pl.ANY)
    smem = pl.BlockSpec(memory_space=pltpu.SMEM)
    dma = pltpu.SemaphoreType.DMA
    outs = tuple(
        pl.pallas_call(
            functools.partial(kernel, chunks, per),
            out_shape=(
                jax.ShapeDtypeStruct((1, tokens, width), BF16),
                jax.ShapeDtypeStruct((1, mine, width), F32),
                jax.ShapeDtypeStruct((1, mine, width), F32),
            ),
            in_specs=[hbm, hbm, hbm, hbm, smem, smem, hbm],
            out_specs=(hbm, hbm, hbm),
            scratch_shapes=[
                pltpu.VMEM((tokens, width), BF16),
                pltpu.VMEM((tokens, width), BF16),
                pltpu.VMEM((tokens,), jnp.int32),
                pltpu.VMEM((2, block, 4 * width), BF16),
                pltpu.VMEM((2, 4, block, width), BF16),
                pltpu.VMEM((tokens, width), BF16),
                pltpu.VMEM((keys // LATENTS, tokens), F32),
                pltpu.VMEM((chunks, 2, 2, NX, part, cw), BF16),
                pltpu.VMEM((chunks, 2, NX, part, cw), BF16),
                pltpu.VMEM((chunks, 2, 2, part, cw), BF16),
                pltpu.VMEM((chunks, 2, 2, part, cw), BF16),
                pltpu.VMEM((chunks, 2, 2, 2, part, cw), BF16),
                pltpu.VMEM((chunks, GROUP, 2 * mine, cw), BF16),
                pltpu.VMEM((chunks, GROUP, 2 * mine, cw), BF16),
                pltpu.VMEM((mine, width), F32),
                pltpu.VMEM((mine, width), F32),
                dma((7,)),
                pltpu.SemaphoreType.REGULAR((4, 2)),
            ]
            + [dma((heads,))] * 6
            + [dma((chunks + 1,))] * 9
            + [dma((chunks + 1, 2))],
            compiler_params=pltpu.CompilerParams(
                collective_id=0, has_side_effects=True, vmem_limit_bytes=60 * 2**20
            ),
            name="attention_grads",
        )(
            queries, visual_keys, visual_values, out_grad, gate_value, image_order,
            image_seen,
        )
    )
    steps = 5
    return tuple(
        pl.pallas_call(
            hand_on,
            out_shape=tuple(jax.ShapeDtypeStruct(o.shape, o.dtype) for o in outs),
            in_specs=[hbm] * 3,
            out_specs=(hbm,) * 3,
            scratch_shapes=[
                pltpu.VMEM((steps, tokens // steps, width), BF16),
                pltpu.VMEM((2, mine, width), F32),
                dma((2, steps + 2)),
            ],
            compiler_params=pltpu.CompilerParams(vmem_limit_bytes=60 * 2**20),
            name="hand_on",
        )(*outs)
    )


def solution(mesh):
    placed = (
        P(None, "txt", "img"),
        P(None, "img", None),
        P(None, "img", None),
        P(None, "txt", "img"),
        P(None, "img"),
        P(),
        P("txt"),
    )
    return jax.shard_map(
        shards,
        mesh=mesh,
        in_specs=placed,
        out_specs=(P(None, "txt", "img"), P(None, "txt", "img"), P(None, "txt", "img")),
        check_vma=False,
    )
```
